256 devices in a mesh: seq: 16 (over x, y_lo, core), emb: 16 (over y_hi, z).
Axes of the slice: x: 4, y: 4 (y_hi: 2, y_lo: 2; y = y_hi * 2 + y_lo), z: 8, core: 2. Of those that a mesh axis runs over, the one named last changes fastest.
Arguments:
- item_ids: int32 [131072], P('seq'), may hold values from 0 to 32767
- domains: int32 [131072], P(('seq', 'emb')), may hold values from 0 to 15, as said below
- live_counts: int32 [256], P(('seq', 'emb')), may hold values from 128 to 512, as said below
- table: bfloat16 [32768, 512], P(None, 'emb'), may hold values from -30 to 30
- norm_gains: float32 [3, 512], replicated, may hold values from 0.25 to 1.75
- proj_in: bfloat16 [512, 2048], replicated, may hold values from -0.25 to 0.25
- proj_out: bfloat16 [512, 512], replicated, may hold values from -0.25 to 0.25
- expert_in: bfloat16 [16, 512, 4096], P('emb'), may hold values from -0.25 to 0.25
- expert_out: bfloat16 [16, 2048, 512], P('emb'), may hold values from -0.125 to 0.125
Outputs:
- mixed: bfloat16 [131072, 512], P(('seq', 'emb'))
The draws below stay inside these ranges and needn't reach their ends.
Inputs may be any that keep to these rules, and one draw needn't show every extreme that they name: `domains`: in the 512 events of one block no domain appears more than 64 times; in every group of 16 consecutive blocks some domain appears exactly 64 times in each block. `live_counts`: some block has all 512 events live.
All inputs are finite; a program needn't handle non-finite values.
Results may differ from the reference program's by a relative error of at most 0.006.
Values may be sent and summed in bfloat16 or wider, within the bound.
A program may use at most 128 MiB of HBM per device.

```python
import math
import jax
import jax.numpy as jnp
import numpy as np
from jax import lax

D = 512
HEADS = 8
HEAD_DIM = 64
HID = 2048
VOCAB = 32768
ROWS = 512
SPAN = 4
EXPERTS = 16
CAP = 64
EVENTS = 131072


def draw_domains(key, part):
    blocks = EVENTS // ROWS
    groups = blocks // EXPERTS
    first, second, third = jax.random.split(jax.random.fold_in(key, 11), 3)
    hot_group = jax.random.randint(first, (groups,), 0, EXPERTS)
    hot = jnp.repeat(hot_group, EXPERTS)
    second_off = jax.random.randint(second, (blocks, 1), 1, EXPERTS)
    remaining = ROWS - CAP
    paired = min(CAP, remaining) // 2
    places = jnp.arange(ROWS, dtype=jnp.int32)[None, :]
    cyclic = 1 + jnp.mod(places - CAP - paired, EXPERTS - 1)
    offset = jnp.where(places < CAP, 0, jnp.where(places < CAP + paired, second_off, cyclic))
    labels = jnp.mod(hot[:, None] + offset, EXPERTS)
    scores = jax.random.randint(third, (blocks, ROWS), 0, 1 << 20) * ROWS + places
    order = jnp.argsort(scores, axis=1, stable=True)
    labels = jnp.take_along_axis(labels, order, axis=1)
    return labels.reshape(EVENTS).astype(jnp.int32)


def draw_live_counts(key, part):
    blocks = EVENTS // ROWS
    first, second = jax.random.split(jax.random.fold_in(key, 23), 2)
    counts = jax.random.randint(first, (blocks,), ROWS // 4, ROWS + 1)
    chosen = jax.random.randint(second, (), 0, blocks)
    counts = jnp.where(jnp.arange(blocks) == chosen, ROWS, counts)
    return counts.astype(jnp.int32)


def draw_table(key, part):
    first, second, third = jax.random.split(jax.random.fold_in(key, 37), 3)
    row_scale = jnp.exp(jax.random.uniform(first, (VOCAB, 1), jnp.float32, math.log(0.3), math.log(3.0)))
    col_scale = jnp.exp(jax.random.uniform(second, (1, D), jnp.float32, math.log(0.5), math.log(2.0)))
    base = jnp.clip(jax.random.normal(third, (VOCAB, D), jnp.float32), -5.0, 5.0)
    return (base * row_scale * col_scale).astype(jnp.bfloat16)


def touch_ends(result, key, least, high):
    shape = result.shape
    spot = [jax.random.randint(jax.random.fold_in(key, axis), (), 0, shape[axis]) for axis in range(len(shape))]
    result = result.at[tuple(spot)].set(least)
    longest = shape.index(max(shape))
    spot[longest] = (spot[longest] + 1) % shape[longest]
    return result.at[tuple(spot)].set(high)


def shard_levels(rng, shape, cuts, low, largest):
    factor_of, own = 1.0, jax.random.fold_in(rng, 6)
    for axis_at, shards_of in cuts:
        steps = jnp.exp(jax.random.uniform(jax.random.fold_in(own, axis_at), (shards_of,), jnp.float32, low / len(cuts), largest / len(cuts)))
        factor_of = factor_of * jnp.repeat(steps, shape[axis_at] // shards_of).reshape([-1 if axis == axis_at else 1 for axis in range(len(shape))])
    return factor_of


def rank_bounds(count, lean):
    portions = [(1 << 20) // math.isqrt(standing ** lean) + 1 for standing in range(1, count + 1)]
    width = 1 + sum(portions) // (1 << 30)
    return np.cumsum(np.array([max(1, weight // width) for weight in portions]))


def ranked_ids(own_key, dims, count, lean):
    listing = rank_bounds(count, lean)
    pick = jax.random.randint(jax.random.fold_in(own_key, 1), dims, 0, int(listing[count - 1]))
    standing = jnp.searchsorted(jnp.asarray(listing, jnp.int32), pick, side="right")
    return jax.random.permutation(jax.random.fold_in(own_key, 2), count)[standing].astype(jnp.int32)


def gaussian(own_key, shape, spread, reach, cuts=(), held_as=jnp.bfloat16):
    drawn = spread * jax.random.normal(own_key, shape, jnp.float32)
    if cuts:
        drawn = drawn * shard_levels(own_key, shape, cuts, -0.22, 0.18)
    return jnp.clip(drawn, -reach, reach).astype(held_as)


def setup_inputs(seed: int = 0) -> dict:
    keys = jax.random.split(jax.random.key(seed), 10)
    return {
        "item_ids": touch_ends(ranked_ids(keys[0], (EVENTS,), VOCAB, 2), jax.random.fold_in(keys[0], 3), 0, VOCAB - 1).astype(jnp.int32),
        "domains": draw_domains(jax.random.fold_in(keys[9], 71), 0),
        "live_counts": draw_live_counts(jax.random.fold_in(keys[9], 71), 0),
        "table": draw_table(jax.random.fold_in(keys[9], 71), 0),
        "norm_gains": jnp.clip(1.0 + 0.15 * jax.random.normal(keys[4], (3, D), jnp.float32), 0.25, 1.75),
        "proj_in": gaussian(keys[5], (D, 4 * D), D ** -0.5, 0.25),
        "proj_out": gaussian(keys[6], (D, D), D ** -0.5, 0.25),
        "expert_in": gaussian(keys[7], (EXPERTS, D, 2 * HID), D ** -0.5, 0.25, ((0, 16),)),
        "expert_out": gaussian(keys[8], (EXPERTS, HID, D), HID ** -0.5, 0.125, ((0, 16),)),
    }


norm_eps = 1e-06

def rms_norm(values, gain):
    return values * lax.rsqrt(lax.optimization_barrier(jnp.mean(values * values, axis=-1, keepdims=True)) + norm_eps) * gain

def reference(item_ids, domains, live_counts, table, norm_gains, proj_in, proj_out, expert_in, expert_out):
    embedded = table[item_ids].astype(jnp.float32)
    positions = jnp.arange(ROWS, dtype=jnp.int32)
    live_mask = (positions[None, :] < live_counts[:, None]).astype(jnp.float32).reshape(EVENTS)
    normed = (rms_norm(embedded, norm_gains[0]) * live_mask[:, None]).astype(jnp.bfloat16)
    projected = jnp.dot(normed, proj_in, preferred_element_type=jnp.float32)
    gating = jax.nn.silu(projected[:, :D])
    queries, key_rows, values = lax.optimization_barrier((projected[:, D:2 * D].astype(jnp.bfloat16), projected[:, 2 * D:3 * D].astype(jnp.bfloat16), projected[:, 3 * D:].astype(jnp.bfloat16)))
    margin = SPAN * ROWS
    window = (2 * SPAN + 1) * ROWS
    key_pad = jnp.pad(key_rows, ((margin, margin), (0, 0)))
    value_pad = jnp.pad(values, ((margin, margin), (0, 0)))
    score_scale = 1.0 / math.sqrt(HEAD_DIM)
    offsets = jnp.arange(ROWS, dtype=jnp.int32)[:, None] + margin - jnp.arange(window, dtype=jnp.int32)[None, :]
    band_mask = (jnp.abs(offsets) <= margin).astype(jnp.float32)

    def one_block(block):
        start = (block * ROWS).astype(jnp.int32)
        query_blk = lax.dynamic_slice_in_dim(queries, start, ROWS, 0).astype(jnp.float32).reshape(ROWS, HEADS, HEAD_DIM)
        key_blk = lax.dynamic_slice_in_dim(key_pad, start, window, 0).astype(jnp.float32).reshape(window, HEADS, HEAD_DIM)
        value_blk = lax.dynamic_slice_in_dim(value_pad, start, window, 0).astype(jnp.float32).reshape(window, HEADS, HEAD_DIM)
        scores = jnp.einsum('qhd,khd->hqk', query_blk, key_blk) * score_scale
        weights = lax.optimization_barrier((jax.nn.silu(scores) * band_mask[None]).astype(jnp.bfloat16))
        return jnp.einsum('hqk,khd->qhd', weights.astype(jnp.float32), value_blk).reshape(ROWS, D)
    attended = lax.map(one_block, jnp.arange(EVENTS // ROWS, dtype=jnp.int32)).reshape(EVENTS, D)
    gated = (rms_norm(attended, norm_gains[1]) * gating).astype(jnp.bfloat16)
    hidden = embedded + jnp.dot(gated, proj_out, preferred_element_type=jnp.float32)
    routed = rms_norm(hidden, norm_gains[2]).astype(jnp.bfloat16)
    bound = CAP * (EVENTS // ROWS)

    def add_expert(expert, total):
        matches = domains == expert
        members = jnp.nonzero(matches, size=bound, fill_value=0)[0].astype(jnp.int32)
        filled = (jnp.arange(bound, dtype=jnp.int32) < jnp.sum(matches.astype(jnp.int32))).astype(jnp.float32)
        chosen = routed[members]
        gate_up = jnp.dot(chosen, expert_in[expert], preferred_element_type=jnp.float32)
        activated = (jax.nn.silu(gate_up[:, :HID]) * gate_up[:, HID:]).astype(jnp.bfloat16)
        produced = lax.optimization_barrier(jnp.dot(activated, expert_out[expert], preferred_element_type=jnp.float32).astype(jnp.bfloat16))
        return total.at[members].add(produced.astype(jnp.float32) * filled[:, None])
    expert_rows = lax.fori_loop(0, EXPERTS, add_expert, jnp.zeros((EVENTS, D), jnp.float32))
    return (live_mask[:, None] * (hidden + expert_rows)).astype(jnp.bfloat16)
```

```python
import math

import jax
import jax.numpy as jnp
from jax import lax
from jax.experimental import pallas as pl
from jax.experimental.pallas import tpu as pltpu
from jax.sharding import PartitionSpec as P

HEADS = 8
HEAD_DIM = 64
SPAN = 4
MESH = pl.DeviceIdType.MESH

norm_eps = 1e-06

ORDER = (4, 12, 3, 13, 5, 11, 2, 14, 6, 10, 1, 15, 7, 9, 8, 0)


def rms_norm(values, gain):
    return values * lax.rsqrt(jnp.mean(values * values, axis=-1, keepdims=True) + norm_eps) * gain


def silu(values):
    return values * (0.5 * jnp.tanh(0.5 * values) + 0.5)


def attention_kernel(
    normed_ref, embedded_ref, gains_ref, proj_in_ref, proj_out_ref, slot_ref,
    hidden_ref, outgoing_ref,
    halo, queries, gating, keys, values, total, send_sem, recv_sem,
):
    rows, width = normed_ref.shape
    half = rows // 2
    pairs = width // 128
    groups, members = lax.axis_size("seq"), lax.axis_size("emb")
    count = groups * members
    me = lax.axis_index("seq") * members + lax.axis_index("emb")
    right = lax.rem(me + 1, count)
    left = lax.rem(me + count - 1, count)
    targets = [
        (lax.div(right, members), lax.rem(right, members)),
        (lax.div(left, members), lax.rem(left, members)),
    ]

    barrier = pltpu.get_barrier_semaphore()
    for target in targets:
        pl.semaphore_signal(barrier, inc=1, device_id=target, device_id_type=MESH)
    pl.semaphore_wait(barrier, 2)

    def transfer(way, distance, part, source):
        slot = (way, distance, part)
        return pltpu.make_async_remote_copy(
            src_ref=source,
            dst_ref=halo.at[slot],
            send_sem=send_sem.at[slot],
            recv_sem=recv_sem.at[slot],
            device_id=targets[way],
            device_id_type=MESH,
        )

    for part in range(2):
        for way in range(2):
            transfer(way, 0, part, normed_ref.at[pl.ds(part * half, half)]).start()

    normed = normed_ref[...]
    for pair in range(pairs):
        columns = pl.ds(pair * 128, 128)
        gate = jnp.dot(normed, proj_in_ref[:, columns], preferred_element_type=jnp.float32)
        gating[:, columns] = silu(gate)
        query = jnp.dot(
            normed, proj_in_ref[:, pl.ds(width + pair * 128, 128)], preferred_element_type=jnp.float32
        ).astype(jnp.bfloat16)
        queries[pair] = query * jnp.bfloat16(0.5 / math.sqrt(HEAD_DIM))
        total[pair] = jnp.zeros((rows, 128), jnp.float32)

    low_lanes = lax.broadcasted_iota(jnp.int32, (half, 128), 1) < HEAD_DIM

    def attend(block, tiles):
        def project(pair, carry):
            for base, held in ((2 * width, keys), (3 * width, values)):
                columns = pl.ds(pl.multiple_of(base + pair * 128, 128), 128)
                found = jnp.dot(block, proj_in_ref[:, columns], preferred_element_type=jnp.float32)
                held[pair, pl.ds(0, half), :] = jnp.where(low_lanes, found, 0.0).astype(jnp.bfloat16)
                held[pair, pl.ds(half, half), :] = jnp.where(low_lanes, 0.0, found).astype(jnp.bfloat16)
            return carry

        lax.fori_loop(0, pairs, project, 0)

        def weigh(pair, carry):
            for tile, band in tiles:
                span = pl.ds(tile * half, half)
                scores = lax.dot_general(
                    queries[pair, span, :], keys[pair], (((1,), (1,)), ((), ())),
                    preferred_element_type=jnp.float32,
                )
                weights = scores * jnp.tanh(scores) + scores
                if band is not None:
                    row = lax.broadcasted_iota(jnp.int32, scores.shape, 0)
                    column = lax.broadcasted_iota(jnp.int32, scores.shape, 1) & (half - 1)
                    weights = jnp.where(column >= row if band == 0 else column <= row, weights, 0.0)
                total[pair, span, :] += jnp.dot(
                    weights.astype(jnp.bfloat16), values[pair], preferred_element_type=jnp.float32
                )
            return carry

        lax.fori_loop(0, pairs, weigh, 0)

    everything = ((0, None), (1, None))

    def own(part, carry):
        attend(normed_ref[pl.ds(pl.multiple_of(part * half, half), half), :], everything)
        return carry

    lax.fori_loop(0, 2, own, 0)

    def in_range(way, distance):
        return me - distance > 0 if way == 0 else me + distance < count - 1

    def step(index, carry):
        distance, part = lax.div(index, 2), lax.rem(index, 2)
        for way in range(2):
            arrived = halo.at[way, distance, part]
            transfer(way, distance, part, arrived).wait_recv()
            transfer(way, distance + 1, part, arrived).start()

        def one(way, carry):
            inside = jnp.where(way == 0, me - distance > 0, me + distance < count - 1)

            @pl.when(inside)
            def _():
                attend(halo[way, distance, part], everything)

            return carry

        lax.fori_loop(0, 2, one, 0)
        return carry

    lax.fori_loop(0, 2 * (SPAN - 1), step, 0)

    last = SPAN - 1
    edge_tiles = (
        (((0, 0),), ((0, 1), (1, None))),
        (((0, None), (1, 0)), ((1, 1),)),
    )
    for part in range(2):
        for way in range(2):
            transfer(way, last, part, halo.at[way, last, part]).wait_recv()

            @pl.when(in_range(way, last))
            def _():
                attend(halo[way, last, part], edge_tiles[part][way])

    def settle(index, carry):
        distance, part = lax.div(index, 2), lax.rem(index, 2)
        for way in range(2):
            transfer(way, distance, part, halo.at[way, distance, part]).wait_send()
        return carry

    lax.fori_loop(0, 2 * SPAN, settle, 0)

    attended = jnp.concatenate([total[pair] for pair in range(pairs)], axis=1)
    gated = (rms_norm(attended, gains_ref[1:2, :]) * gating[...]).astype(jnp.bfloat16)
    hidden = embedded_ref[...].astype(jnp.float32) + jnp.dot(
        gated, proj_out_ref[...], preferred_element_type=jnp.float32
    )
    hidden_ref[...] = hidden
    routed = rms_norm(hidden, gains_ref[2:3, :]).astype(jnp.bfloat16)
    slots = outgoing_ref.shape[0]
    chunk = 256
    for first in range(0, slots, chunk):
        number = lax.broadcasted_iota(jnp.int32, (chunk, rows), 0) + first
        chosen = jnp.where(number == slot_ref[...], 1.0, 0.0).astype(jnp.bfloat16)
        outgoing_ref[pl.ds(first, chunk), :] = jnp.dot(
            chosen, routed, preferred_element_type=jnp.float32
        ).astype(jnp.bfloat16)


def expert_kernel(
    live_ref, outgoing_ref, slot_ref, hidden_ref, expert_in_ref, expert_out_ref,
    mixed_ref,
    up, down, inbox, finished, returned, load_sem, send_sem, recv_sem, back_send, back_recv,
):
    members, capacity, width = outgoing_ref.shape
    hidden_units = down.shape[0]
    rows = hidden_ref.shape[0]
    group = lax.axis_index("seq")
    me = lax.axis_index("emb")

    loads = [
        pltpu.make_async_copy(expert_in_ref.at[0], up, load_sem.at[0]),
        pltpu.make_async_copy(expert_out_ref.at[0], down, load_sem.at[1]),
    ]
    for load in loads:
        load.start()

    barrier = pltpu.get_barrier_semaphore()
    for offset in range(1, members):
        pl.semaphore_signal(
            barrier, inc=1, device_id=(group, lax.rem(me + offset, members)), device_id_type=MESH
        )
    pl.semaphore_wait(barrier, members - 1)

    def dispatch(place):
        target = lax.rem(me + ORDER[place], members)
        return pltpu.make_async_remote_copy(
            src_ref=outgoing_ref.at[target],
            dst_ref=inbox.at[place],
            send_sem=send_sem.at[place],
            recv_sem=recv_sem.at[place],
            device_id=(group, target),
            device_id_type=MESH,
        )

    def give_back(place):
        target = lax.rem(me + members - ORDER[place], members)
        return pltpu.make_async_remote_copy(
            src_ref=finished.at[place],
            dst_ref=returned.at[me],
            send_sem=back_send.at[place],
            recv_sem=back_recv.at[place],
            device_id=(group, target),
            device_id_type=MESH,
        )

    remote = [place for place in range(members) if ORDER[place] != 0]
    home = ORDER.index(0)
    for place in remote:
        dispatch(place).start()
    inbox[home] = outgoing_ref[me]

    batch = 4
    tile = 256
    for load in loads:
        load.wait()
    for first in range(0, members, batch):
        places = [place for place in range(first, first + batch) if place != home]
        for place in places:
            dispatch(place).wait_recv()
        taken = inbox[pl.ds(first, batch)].reshape(batch * capacity, width)

        def expert(index, result):
            start = pl.multiple_of(index * tile, tile)
            gate = jnp.dot(taken, up[:, pl.ds(start, tile)], preferred_element_type=jnp.float32)
            lift = jnp.dot(
                taken, up[:, pl.ds(pl.multiple_of(hidden_units + start, tile), tile)],
                preferred_element_type=jnp.float32,
            )
            activated = (silu(gate) * lift).astype(jnp.bfloat16)
            return result + jnp.dot(
                activated, down[pl.ds(start, tile), :], preferred_element_type=jnp.float32
            )

        produced = lax.fori_loop(
            0, hidden_units // tile, expert, jnp.zeros((batch * capacity, width), jnp.float32)
        ).astype(jnp.bfloat16)
        finished[pl.ds(first, batch)] = produced.reshape(batch, capacity, width)
        for place in places:
            give_back(place).start()

    returned[me] = finished[home]
    for place in remote:
        give_back(place).wait_recv()

    number = lax.broadcasted_iota(jnp.int32, (rows, members * capacity), 1)
    chosen = jnp.where(number == slot_ref[...], 1.0, 0.0).astype(jnp.bfloat16)
    expert_rows = jnp.dot(
        chosen, returned[...].reshape(members * capacity, width), preferred_element_type=jnp.float32
    )
    live = lax.broadcasted_iota(jnp.int32, (rows, width), 0) < live_ref[0]
    mixed_ref[...] = jnp.where(live, hidden_ref[...] + expert_rows, 0.0).astype(jnp.bfloat16)
    for place in remote:
        dispatch(place).wait_send()
        give_back(place).wait_send()


VMEM = pl.BlockSpec(memory_space=pltpu.VMEM)


def body(
    item_ids, domains, live_counts, table, norm_gains, proj_in, proj_out, expert_in, expert_out
):
    rows = domains.shape[0]
    width = proj_out.shape[0]
    hidden_units = expert_out.shape[1]
    members = lax.axis_size("emb")
    capacity = 2 * rows // members
    slots = members * capacity

    onehot_domain = (domains[:, None] == jnp.arange(members, dtype=jnp.int32)[None, :]).astype(jnp.int32)
    slot_rank = jnp.sum((jnp.cumsum(onehot_domain, axis=0) - onehot_domain) * onehot_domain, axis=1)
    slot_index = domains * capacity + slot_rank

    columns = table[item_ids]
    embedded = lax.all_to_all(columns, "emb", split_axis=0, concat_axis=1, tiled=True)
    positions = jnp.arange(rows, dtype=jnp.int32)
    live_mask = (positions < live_counts[0]).astype(jnp.float32)
    normed = (rms_norm(embedded.astype(jnp.float32), norm_gains[0]) * live_mask[:, None]).astype(jnp.bfloat16)

    half = rows // 2
    pairs = width // 128
    hidden, outgoing = pl.pallas_call(
        attention_kernel,
        out_shape=(
            jax.ShapeDtypeStruct((rows, width), jnp.float32),
            jax.ShapeDtypeStruct((slots, width), jnp.bfloat16),
        ),
        in_specs=[VMEM] * 6,
        out_specs=(VMEM, VMEM),
        scratch_shapes=[
            pltpu.VMEM((2, SPAN, 2, half, width), jnp.bfloat16),
            pltpu.VMEM((pairs, rows, 128), jnp.bfloat16),
            pltpu.VMEM((rows, width), jnp.float32),
            pltpu.VMEM((pairs, rows, 128), jnp.bfloat16),
            pltpu.VMEM((pairs, rows, 128), jnp.bfloat16),
            pltpu.VMEM((pairs, rows, 128), jnp.float32),
            pltpu.SemaphoreType.DMA((2, SPAN, 2)),
            pltpu.SemaphoreType.DMA((2, SPAN, 2)),
        ],
        compiler_params=pltpu.CompilerParams(
            collective_id=0, has_side_effects=True, vmem_limit_bytes=40 << 20
        ),
        name="attention",
    )(normed, embedded, norm_gains, proj_in, proj_out, slot_index[None, :])

    return pl.pallas_call(
        expert_kernel,
        out_shape=jax.ShapeDtypeStruct((rows, width), jnp.bfloat16),
        in_specs=[
            pl.BlockSpec(memory_space=pltpu.SMEM), VMEM, VMEM, VMEM,
            pl.BlockSpec(memory_space=pl.ANY), pl.BlockSpec(memory_space=pl.ANY),
        ],
        out_specs=VMEM,
        scratch_shapes=[
            pltpu.VMEM((width, 2 * hidden_units), jnp.bfloat16),
            pltpu.VMEM((hidden_units, width), jnp.bfloat16),
            pltpu.VMEM((members, capacity, width), jnp.bfloat16),
            pltpu.VMEM((members, capacity, width), jnp.bfloat16),
            pltpu.VMEM((members, capacity, width), jnp.bfloat16),
            pltpu.SemaphoreType.DMA((2,)),
            pltpu.SemaphoreType.DMA((members,)),
            pltpu.SemaphoreType.DMA((members,)),
            pltpu.SemaphoreType.DMA((members,)),
            pltpu.SemaphoreType.DMA((members,)),
        ],
        compiler_params=pltpu.CompilerParams(
            collective_id=1, has_side_effects=True, vmem_limit_bytes=40 << 20
        ),
        name="experts",
    )(
        live_counts, outgoing.reshape(members, capacity, width), slot_index[:, None], hidden,
        expert_in, expert_out,
    )


def solution(mesh):
    in_specs = (
        P("seq"),
        P(("seq", "emb")),
        P(("seq", "emb")),
        P(None, "emb"),
        P(),
        P(),
        P(),
        P("emb", None, None),
        P("emb", None, None),
    )
    out_specs = P(("seq", "emb"), None)
    return jax.shard_map(body, mesh=mesh, in_specs=in_specs, out_specs=out_specs, check_vma=False)
```

```python
import math

import jax
import jax.numpy as jnp
from jax import lax
from jax.experimental import pallas as pl
from jax.experimental.pallas import tpu as pltpu
from jax.sharding import PartitionSpec as P

HEADS = 8
HEAD_DIM = 64
SPAN = 4
MESH = pl.DeviceIdType.MESH

norm_eps = 1e-06

ORDER = (4, 12, 3, 13, 5, 11, 2, 14, 6, 10, 1, 15, 7, 9, 8, 0)


def rms_norm(values, gain):
    return values * lax.rsqrt(jnp.mean(values * values, axis=-1, keepdims=True) + norm_eps) * gain


def silu(values):
    return values * (0.5 * jnp.tanh(0.5 * values) + 0.5)


def attention_kernel(
    normed_ref, embedded_ref, gains_ref, proj_in_ref, proj_out_ref, slot_ref,
    hidden_ref, outgoing_ref,
    halo, queries, gating, keys, values, total, send_sem, recv_sem,
):
    rows, width = normed_ref.shape
    half = rows // 2
    pairs = width // 128
    groups, members = lax.axis_size("seq"), lax.axis_size("emb")
    count = groups * members
    me = lax.axis_index("seq") * members + lax.axis_index("emb")
    right = lax.rem(me + 1, count)
    left = lax.rem(me + count - 1, count)
    targets = [
        (lax.div(right, members), lax.rem(right, members)),
        (lax.div(left, members), lax.rem(left, members)),
    ]

    barrier = pltpu.get_barrier_semaphore()
    for target in targets:
        pl.semaphore_signal(barrier, inc=1, device_id=target, device_id_type=MESH)
    pl.semaphore_wait(barrier, 2)

    def transfer(way, distance, part, source):
        slot = (way, distance, part)
        return pltpu.make_async_remote_copy(
            src_ref=source,
            dst_ref=halo.at[slot],
            send_sem=send_sem.at[slot],
            recv_sem=recv_sem.at[slot],
            device_id=targets[way],
            device_id_type=MESH,
        )

    for part in range(2):
        for way in range(2):
            transfer(way, 0, part, normed_ref.at[pl.ds(part * half, half)]).start()

    normed = normed_ref[...]
    for pair in range(pairs):
        columns = pl.ds(pair * 128, 128)
        gate = jnp.dot(normed, proj_in_ref[:, columns], preferred_element_type=jnp.float32)
        gating[:, columns] = silu(gate)
        query = jnp.dot(
            normed, proj_in_ref[:, pl.ds(width + pair * 128, 128)], preferred_element_type=jnp.float32
        ).astype(jnp.bfloat16)
        queries[pair] = query * jnp.bfloat16(0.5 / math.sqrt(HEAD_DIM))
        total[pair] = jnp.zeros((rows, 128), jnp.float32)

    low_lanes = lax.broadcasted_iota(jnp.int32, (half, 128), 1) < HEAD_DIM

    def attend(block, tiles):
        def project(group, carry):
            for base, held in ((2 * width, keys), (3 * width, values)):
                columns = pl.ds(pl.multiple_of(base + group * 256, 256), 256)
                found = jnp.dot(block, proj_in_ref[:, columns], preferred_element_type=jnp.float32)
                for side in range(2):
                    pair = 2 * group + side
                    mine = found[:, side * 128 : (side + 1) * 128]
                    held[pair, pl.ds(0, half), :] = jnp.where(low_lanes, mine, 0.0).astype(jnp.bfloat16)
                    held[pair, pl.ds(half, half), :] = jnp.where(low_lanes, 0.0, mine).astype(jnp.bfloat16)
            return carry

        lax.fori_loop(0, pairs // 2, project, 0)

        def weigh(pair, carry):
            for tile, band in tiles:
                span = pl.ds(tile * half, half)
                scores = lax.dot_general(
                    queries[pair, span, :], keys[pair], (((1,), (1,)), ((), ())),
                    preferred_element_type=jnp.float32,
                )
                weights = scores * jnp.tanh(scores) + scores
                if band is not None:
                    row = lax.broadcasted_iota(jnp.int32, scores.shape, 0)
                    column = lax.broadcasted_iota(jnp.int32, scores.shape, 1) & (half - 1)
                    weights = jnp.where(column >= row if band == 0 else column <= row, weights, 0.0)
                total[pair, span, :] += jnp.dot(
                    weights.astype(jnp.bfloat16), values[pair], preferred_element_type=jnp.float32
                )
            return carry

        lax.fori_loop(0, pairs, weigh, 0)

    everything = ((0, None), (1, None))

    def own(part, carry):
        attend(normed_ref[pl.ds(pl.multiple_of(part * half, half), half), :], everything)
        return carry

    lax.fori_loop(0, 2, own, 0)

    def in_range(way, distance):
        return me - distance > 0 if way == 0 else me + distance < count - 1

    def step(index, carry):
        distance, part = lax.div(index, 2), lax.rem(index, 2)
        def one(way, carry):
            for side in range(2):

                @pl.when(way == side)
                def _():
                    arrived = halo.at[side, distance, part]
                    transfer(side, distance, part, arrived).wait_recv()
                    transfer(side, distance + 1, part, arrived).start()

            inside = jnp.where(way == 0, me - distance > 0, me + distance < count - 1)

            @pl.when(inside)
            def _():
                attend(halo[way, distance, part], everything)

            return carry

        lax.fori_loop(0, 2, one, 0)
        return carry

    lax.fori_loop(0, 2 * (SPAN - 1), step, 0)

    last = SPAN - 1
    edge_tiles = (
        (((0, 0),), ((0, 1), (1, None))),
        (((0, None), (1, 0)), ((1, 1),)),
    )
    for part in range(2):
        for way in range(2):
            transfer(way, last, part, halo.at[way, last, part]).wait_recv()

            @pl.when(in_range(way, last))
            def _():
                attend(halo[way, last, part], edge_tiles[part][way])

    def settle(index, carry):
        distance, part = lax.div(index, 2), lax.rem(index, 2)
        for way in range(2):
            transfer(way, distance, part, halo.at[way, distance, part]).wait_send()
        return carry

    lax.fori_loop(0, 2 * SPAN, settle, 0)

    attended = jnp.concatenate([total[pair] for pair in range(pairs)], axis=1)
    gated = (rms_norm(attended, gains_ref[1:2, :]) * gating[...]).astype(jnp.bfloat16)
    hidden = embedded_ref[...].astype(jnp.float32) + jnp.dot(
        gated, proj_out_ref[...], preferred_element_type=jnp.float32
    )
    hidden_ref[...] = hidden
    routed = rms_norm(hidden, gains_ref[2:3, :]).astype(jnp.bfloat16)
    slots = outgoing_ref.shape[0]
    chunk = 256
    for first in range(0, slots, chunk):
        number = lax.broadcasted_iota(jnp.int32, (chunk, rows), 0) + first
        chosen = jnp.where(number == slot_ref[...], 1.0, 0.0).astype(jnp.bfloat16)
        outgoing_ref[pl.ds(first, chunk), :] = jnp.dot(
            chosen, routed, preferred_element_type=jnp.float32
        ).astype(jnp.bfloat16)


def expert_kernel(
    live_ref, outgoing_ref, slot_ref, hidden_ref, expert_in_ref, expert_out_ref,
    mixed_ref,
    up, down, inbox, finished, returned, load_sem, send_sem, recv_sem, back_send, back_recv,
):
    members, capacity, width = outgoing_ref.shape
    hidden_units = down.shape[0]
    rows = hidden_ref.shape[0]
    group = lax.axis_index("seq")
    me = lax.axis_index("emb")

    loads = [
        pltpu.make_async_copy(expert_in_ref.at[0], up, load_sem.at[0]),
        pltpu.make_async_copy(expert_out_ref.at[0], down, load_sem.at[1]),
    ]
    for load in loads:
        load.start()

    barrier = pltpu.get_barrier_semaphore()
    for offset in range(1, members):
        pl.semaphore_signal(
            barrier, inc=1, device_id=(group, lax.rem(me + offset, members)), device_id_type=MESH
        )
    pl.semaphore_wait(barrier, members - 1)

    def dispatch(place):
        target = lax.rem(me + ORDER[place], members)
        return pltpu.make_async_remote_copy(
            src_ref=outgoing_ref.at[target],
            dst_ref=inbox.at[place],
            send_sem=send_sem.at[place],
            recv_sem=recv_sem.at[place],
            device_id=(group, target),
            device_id_type=MESH,
        )

    def give_back(place):
        target = lax.rem(me + members - ORDER[place], members)
        return pltpu.make_async_remote_copy(
            src_ref=finished.at[place],
            dst_ref=returned.at[me],
            send_sem=back_send.at[place],
            recv_sem=back_recv.at[place],
            device_id=(group, target),
            device_id_type=MESH,
        )

    remote = [place for place in range(members) if ORDER[place] != 0]
    home = ORDER.index(0)
    for place in remote:
        dispatch(place).start()
    inbox[home] = outgoing_ref[me]

    batch = 4
    tile = 256
    for load in loads:
        load.wait()
    for first in range(0, members, batch):
        places = [place for place in range(first, first + batch) if place != home]
        for place in places:
            dispatch(place).wait_recv()
        taken = inbox[pl.ds(first, batch)].reshape(batch * capacity, width)

        def expert(index, result):
            start = pl.multiple_of(index * tile, tile)
            gate = jnp.dot(taken, up[:, pl.ds(start, tile)], preferred_element_type=jnp.float32)
            lift = jnp.dot(
                taken, up[:, pl.ds(pl.multiple_of(hidden_units + start, tile), tile)],
                preferred_element_type=jnp.float32,
            )
            activated = (silu(gate) * lift).astype(jnp.bfloat16)
            return result + jnp.dot(
                activated, down[pl.ds(start, tile), :], preferred_element_type=jnp.float32
            )

        produced = lax.fori_loop(
            0, hidden_units // tile, expert, jnp.zeros((batch * capacity, width), jnp.float32)
        ).astype(jnp.bfloat16)
        finished[pl.ds(first, batch)] = produced.reshape(batch, capacity, width)
        for place in places:
            give_back(place).start()

    returned[me] = finished[home]
    for place in remote:
        give_back(place).wait_recv()

    number = lax.broadcasted_iota(jnp.int32, (rows, members * capacity), 1)
    chosen = jnp.where(number == slot_ref[...], 1.0, 0.0).astype(jnp.bfloat16)
    expert_rows = jnp.dot(
        chosen, returned[...].reshape(members * capacity, width), preferred_element_type=jnp.float32
    )
    live = lax.broadcasted_iota(jnp.int32, (rows, width), 0) < live_ref[0]
    mixed_ref[...] = jnp.where(live, hidden_ref[...] + expert_rows, 0.0).astype(jnp.bfloat16)
    for place in remote:
        dispatch(place).wait_send()
        give_back(place).wait_send()


def gather_kernel(place_ref, table_ref, outgoing_ref, spread, stage):
    features, vocabulary = table_ref.shape
    copies = 128 // features
    depth = vocabulary // copies
    members, lines, _ = outgoing_ref.shape

    def arrange(index, carry):
        start = pl.multiple_of(index * 128, 128)
        stacked = jnp.concatenate(
            [table_ref[:, pl.ds(pl.multiple_of(k * depth + start, 128), 128)] for k in range(copies)], axis=0
        )
        turned = stacked.astype(jnp.float32).T
        for shift in range(copies):
            moved = turned if shift == 0 else pltpu.roll(turned, shift * features, 1)
            spread[pl.ds(pl.multiple_of(shift * depth + start, 128), 128), :] = moved
        return carry

    lax.fori_loop(0, depth // 128, arrange, 0)

    lane = lax.broadcasted_iota(jnp.int32, (1, 128), 1)
    inside = [lane < (k + 1) * features for k in range(copies - 1)]

    def member(target, carry):
        def eight(index, carry):
            first = target * (copies * lines) + index * 8
            for line in range(8):
                found = [
                    spread[pl.ds(place_ref[first + k * lines + line], 1), :] for k in range(copies)
                ]
                row = found[-1]
                for k in reversed(range(copies - 1)):
                    row = jnp.where(inside[k], found[k], row)
                stage[pl.ds(index * 8 + line, 1), :] = row
            return carry

        lax.fori_loop(0, lines // 8, eight, 0)
        outgoing_ref[target] = stage[...].astype(jnp.bfloat16)
        return carry

    lax.fori_loop(0, members, member, 0)


def exchange_kernel(live_ref, outgoing_ref, gains_ref, embedded_ref, normed_ref, inbox, send_sem, recv_sem):
    members, lines, _ = outgoing_ref.shape
    width = embedded_ref.shape[1]
    features = width // members
    copies = 128 // features
    group = lax.axis_index("seq")
    me = lax.axis_index("emb")

    barrier = pltpu.get_barrier_semaphore()
    for offset in range(1, members):
        pl.semaphore_signal(
            barrier, inc=1, device_id=(group, lax.rem(me + offset, members)), device_id_type=MESH
        )
    pl.semaphore_wait(barrier, members - 1)

    def transfer(place):
        target = lax.rem(me + ORDER[place], members)
        return pltpu.make_async_remote_copy(
            src_ref=outgoing_ref.at[target],
            dst_ref=inbox.at[me],
            send_sem=send_sem.at[place],
            recv_sem=recv_sem.at[place],
            device_id=(group, target),
            device_id_type=MESH,
        )

    remote = [place for place in range(members) if ORDER[place] != 0]
    for place in remote:
        transfer(place).start()
    inbox[me] = outgoing_ref[me]
    for place in remote:
        transfer(place).wait_recv()

    lane = lax.broadcasted_iota(jnp.int32, (lines, 128), 1)
    row = lax.broadcasted_iota(jnp.int32, (lines, 1), 0)
    for part in range(copies):
        blocks = []
        for column in range(width // 128):
            joined = None
            for k in reversed(range(copies)):
                piece = inbox[column * copies + k].astype(jnp.float32)
                shift = (k - part) % copies
                if shift:
                    piece = pltpu.roll(piece, shift * features, 1)
                joined = piece if joined is None else jnp.where(lane < (k + 1) * features, piece, joined)
            blocks.append(joined)
        values = jnp.concatenate(blocks, axis=1)
        span = pl.ds(part * lines, lines)
        embedded_ref[span, :] = values.astype(jnp.bfloat16)
        live = jnp.where(row + part * lines < live_ref[0], 1.0, 0.0)
        normed_ref[span, :] = (rms_norm(values, gains_ref[0:1, :]) * live).astype(jnp.bfloat16)
    for place in remote:
        transfer(place).wait_send()


VMEM = pl.BlockSpec(memory_space=pltpu.VMEM)
SMEM = pl.BlockSpec(memory_space=pltpu.SMEM)


def body(
    item_ids, domains, live_counts, table, norm_gains, proj_in, proj_out, expert_in, expert_out
):
    rows = domains.shape[0]
    width = proj_out.shape[0]
    hidden_units = expert_out.shape[1]
    members = lax.axis_size("emb")
    capacity = 2 * rows // members
    slots = members * capacity

    onehot_domain = (domains[:, None] == jnp.arange(members, dtype=jnp.int32)[None, :]).astype(jnp.int32)
    slot_rank = jnp.sum((jnp.cumsum(onehot_domain, axis=0) - onehot_domain) * onehot_domain, axis=1)
    slot_index = domains * capacity + slot_rank

    vocabulary, features = table.shape
    copies = 128 // features
    depth = vocabulary // copies
    lines = rows // copies
    quarter = (jnp.arange(item_ids.shape[0], dtype=jnp.int32) // lines) % copies
    place = ((quarter - item_ids // depth) % copies) * depth + item_ids % depth
    columns = pl.pallas_call(
        gather_kernel,
        out_shape=jax.ShapeDtypeStruct((members, lines, 128), jnp.bfloat16),
        in_specs=[SMEM, VMEM],
        out_specs=VMEM,
        scratch_shapes=[
            pltpu.VMEM((copies * depth, 128), jnp.float32),
            pltpu.VMEM((lines, 128), jnp.float32),
        ],
        compiler_params=pltpu.CompilerParams(vmem_limit_bytes=32 << 20),
        name="gather",
    )(place, table.T)
    embedded, normed = pl.pallas_call(
        exchange_kernel,
        out_shape=(jax.ShapeDtypeStruct((rows, width), jnp.bfloat16),) * 2,
        in_specs=[SMEM, VMEM, VMEM],
        out_specs=(VMEM, VMEM),
        scratch_shapes=[
            pltpu.VMEM((members, lines, 128), jnp.bfloat16),
            pltpu.SemaphoreType.DMA((members,)),
            pltpu.SemaphoreType.DMA((members,)),
        ],
        compiler_params=pltpu.CompilerParams(
            collective_id=2, has_side_effects=True, vmem_limit_bytes=40 << 20
        ),
        name="exchange",
    )(live_counts, columns, norm_gains)

    half = rows // 2
    pairs = width // 128
    hidden, outgoing = pl.pallas_call(
        attention_kernel,
        out_shape=(
            jax.ShapeDtypeStruct((rows, width), jnp.float32),
            jax.ShapeDtypeStruct((slots, width), jnp.bfloat16),
        ),
        in_specs=[VMEM] * 6,
        out_specs=(VMEM, VMEM),
        scratch_shapes=[
            pltpu.VMEM((2, SPAN, 2, half, width), jnp.bfloat16),
            pltpu.VMEM((pairs, rows, 128), jnp.bfloat16),
            pltpu.VMEM((rows, width), jnp.float32),
            pltpu.VMEM((pairs, rows, 128), jnp.bfloat16),
            pltpu.VMEM((pairs, rows, 128), jnp.bfloat16),
            pltpu.VMEM((pairs, rows, 128), jnp.float32),
            pltpu.SemaphoreType.DMA((2, SPAN, 2)),
            pltpu.SemaphoreType.DMA((2, SPAN, 2)),
        ],
        compiler_params=pltpu.CompilerParams(
            collective_id=0, has_side_effects=True, vmem_limit_bytes=40 << 20
        ),
        name="attention",
    )(normed, embedded, norm_gains, proj_in, proj_out, slot_index[None, :])

    return pl.pallas_call(
        expert_kernel,
        out_shape=jax.ShapeDtypeStruct((rows, width), jnp.bfloat16),
        in_specs=[
            pl.BlockSpec(memory_space=pltpu.SMEM), VMEM, VMEM, VMEM,
            pl.BlockSpec(memory_space=pl.ANY), pl.BlockSpec(memory_space=pl.ANY),
        ],
        out_specs=VMEM,
        scratch_shapes=[
            pltpu.VMEM((width, 2 * hidden_units), jnp.bfloat16),
            pltpu.VMEM((hidden_units, width), jnp.bfloat16),
            pltpu.VMEM((members, capacity, width), jnp.bfloat16),
            pltpu.VMEM((members, capacity, width), jnp.bfloat16),
            pltpu.VMEM((members, capacity, width), jnp.bfloat16),
            pltpu.SemaphoreType.DMA((2,)),
            pltpu.SemaphoreType.DMA((members,)),
            pltpu.SemaphoreType.DMA((members,)),
            pltpu.SemaphoreType.DMA((members,)),
            pltpu.SemaphoreType.DMA((members,)),
        ],
        compiler_params=pltpu.CompilerParams(
            collective_id=1, has_side_effects=True, vmem_limit_bytes=40 << 20
        ),
        name="experts",
    )(
        live_counts, outgoing.reshape(members, capacity, width), slot_index[:, None], hidden,
        expert_in, expert_out,
    )


def solution(mesh):
    in_specs = (
        P("seq"),
        P(("seq", "emb")),
        P(("seq", "emb")),
        P(None, "emb"),
        P(),
        P(),
        P(),
        P("emb", None, None),
        P("emb", None, None),
    )
    out_specs = P(("seq", "emb"), None)
    return jax.shard_map(body, mesh=mesh, in_specs=in_specs, out_specs=out_specs, check_vma=False)
```

```python
import math

import jax
import jax.numpy as jnp
from jax import lax
from jax.experimental import pallas as pl
from jax.experimental.pallas import tpu as pltpu
from jax.sharding import PartitionSpec as P

HEADS = 8
HEAD_DIM = 64
SPAN = 4
MESH = pl.DeviceIdType.MESH

norm_eps = 1e-06

ORDER = (4, 12, 3, 13, 5, 11, 2, 14, 6, 10, 1, 15, 7, 9, 8, 0)


def rms_norm(values, gain):
    return values * lax.rsqrt(jnp.mean(values * values, axis=-1, keepdims=True) + norm_eps) * gain


def silu(values):
    return values * (0.5 * jnp.tanh(0.5 * values) + 0.5)


def slot_numbers(domains, members, capacity):
    rows = domains.shape[1]
    onehot = jnp.where(lax.broadcasted_iota(jnp.int32, (members, rows), 0) == domains, 1.0, 0.0)
    before = jnp.where(
        lax.broadcasted_iota(jnp.int32, (rows, rows), 0) < lax.broadcasted_iota(jnp.int32, (rows, rows), 1),
        1.0, 0.0,
    )
    ranks = jnp.dot(
        onehot.astype(jnp.bfloat16), before.astype(jnp.bfloat16), preferred_element_type=jnp.float32
    )
    rank = jnp.sum(ranks * onehot, axis=0, keepdims=True)
    return domains.astype(jnp.float32) * capacity + rank


def attention_kernel(
    normed_ref, embedded_ref, gains_ref, proj_in_ref, proj_out_ref, domains_ref,
    hidden_ref, outgoing_ref,
    halo, queries, gating, keys, values, total, send_sem, recv_sem,
):
    rows, width = normed_ref.shape
    half = rows // 2
    pairs = width // 128
    groups, members = lax.axis_size("seq"), lax.axis_size("emb")
    count = groups * members
    me = lax.axis_index("seq") * members + lax.axis_index("emb")
    right = lax.rem(me + 1, count)
    left = lax.rem(me + count - 1, count)
    targets = [
        (lax.div(right, members), lax.rem(right, members)),
        (lax.div(left, members), lax.rem(left, members)),
    ]

    barrier = pltpu.get_barrier_semaphore()
    for target in targets:
        pl.semaphore_signal(barrier, inc=1, device_id=target, device_id_type=MESH)
    pl.semaphore_wait(barrier, 2)

    def transfer(way, distance, part, source):
        slot = (way, distance, part)
        return pltpu.make_async_remote_copy(
            src_ref=source,
            dst_ref=halo.at[slot],
            send_sem=send_sem.at[slot],
            recv_sem=recv_sem.at[slot],
            device_id=targets[way],
            device_id_type=MESH,
        )

    for part in range(2):
        for way in range(2):
            transfer(way, 0, part, normed_ref.at[pl.ds(part * half, half)]).start()

    normed = normed_ref[...]
    for pair in range(pairs):
        columns = pl.ds(pair * 128, 128)
        gate = jnp.dot(normed, proj_in_ref[:, columns], preferred_element_type=jnp.float32)
        gating[:, columns] = silu(gate)
        query = jnp.dot(
            normed, proj_in_ref[:, pl.ds(width + pair * 128, 128)], preferred_element_type=jnp.float32
        ).astype(jnp.bfloat16)
        queries[pair] = query * jnp.bfloat16(0.5 / math.sqrt(HEAD_DIM))
        total[pair] = jnp.zeros((rows, 128), jnp.float32)

    slot_row = slot_numbers(domains_ref[...], members, outgoing_ref.shape[0] // members).astype(jnp.int32)
    low_lanes = lax.broadcasted_iota(jnp.int32, (half, 128), 1) < HEAD_DIM

    def attend(block, tiles):
        def project(group, carry):
            for base, held in ((2 * width, keys), (3 * width, values)):
                columns = pl.ds(pl.multiple_of(base + group * 256, 256), 256)
                found = jnp.dot(block, proj_in_ref[:, columns], preferred_element_type=jnp.float32)
                for side in range(2):
                    pair = 2 * group + side
                    mine = found[:, side * 128 : (side + 1) * 128]
                    held[pair, pl.ds(0, half), :] = jnp.where(low_lanes, mine, 0.0).astype(jnp.bfloat16)
                    held[pair, pl.ds(half, half), :] = jnp.where(low_lanes, 0.0, mine).astype(jnp.bfloat16)
            return carry

        lax.fori_loop(0, pairs // 2, project, 0)

        def weigh(pair, carry):
            for tile, band in tiles:
                span = pl.ds(tile * half, half)
                scores = lax.dot_general(
                    queries[pair, span, :], keys[pair], (((1,), (1,)), ((), ())),
                    preferred_element_type=jnp.float32,
                )
                weights = scores * jnp.tanh(scores) + scores
                if band is not None:
                    row = lax.broadcasted_iota(jnp.int32, scores.shape, 0)
                    column = lax.broadcasted_iota(jnp.int32, scores.shape, 1) & (half - 1)
                    weights = jnp.where(column >= row if band == 0 else column <= row, weights, 0.0)
                total[pair, span, :] += jnp.dot(
                    weights.astype(jnp.bfloat16), values[pair], preferred_element_type=jnp.float32
                )
            return carry

        lax.fori_loop(0, pairs, weigh, 0)

    everything = ((0, None), (1, None))

    def own(part, carry):
        attend(normed_ref[pl.ds(pl.multiple_of(part * half, half), half), :], everything)
        return carry

    lax.fori_loop(0, 2, own, 0)

    def in_range(way, distance):
        return me - distance > 0 if way == 0 else me + distance < count - 1

    def step(index, carry):
        distance, part = lax.div(index, 2), lax.rem(index, 2)
        def one(way, carry):
            for side in range(2):

                @pl.when(way == side)
                def _():
                    arrived = halo.at[side, distance, part]
                    transfer(side, distance, part, arrived).wait_recv()
                    transfer(side, distance + 1, part, arrived).start()

            inside = jnp.where(way == 0, me - distance > 0, me + distance < count - 1)

            @pl.when(inside)
            def _():
                attend(halo[way, distance, part], everything)

            return carry

        lax.fori_loop(0, 2, one, 0)
        return carry

    lax.fori_loop(0, 2 * (SPAN - 1), step, 0)

    last = SPAN - 1
    edge_tiles = (
        (((0, 0),), ((0, 1), (1, None))),
        (((0, None), (1, 0)), ((1, 1),)),
    )
    for part in range(2):
        for way in range(2):
            transfer(way, last, part, halo.at[way, last, part]).wait_recv()

            @pl.when(in_range(way, last))
            def _():
                attend(halo[way, last, part], edge_tiles[part][way])

    def settle(index, carry):
        distance, part = lax.div(index, 2), lax.rem(index, 2)
        for way in range(2):
            transfer(way, distance, part, halo.at[way, distance, part]).wait_send()
        return carry

    lax.fori_loop(0, 2 * SPAN, settle, 0)

    attended = jnp.concatenate([total[pair] for pair in range(pairs)], axis=1)
    gated = (rms_norm(attended, gains_ref[1:2, :]) * gating[...]).astype(jnp.bfloat16)
    hidden = embedded_ref[...].astype(jnp.float32) + jnp.dot(
        gated, proj_out_ref[...], preferred_element_type=jnp.float32
    )
    hidden_ref[...] = hidden
    routed = rms_norm(hidden, gains_ref[2:3, :]).astype(jnp.bfloat16)
    slots = outgoing_ref.shape[0]
    chunk = 256
    for first in range(0, slots, chunk):
        number = lax.broadcasted_iota(jnp.int32, (chunk, rows), 0) + first
        chosen = jnp.where(number == slot_row, 1.0, 0.0).astype(jnp.bfloat16)
        outgoing_ref[pl.ds(first, chunk), :] = jnp.dot(
            chosen, routed, preferred_element_type=jnp.float32
        ).astype(jnp.bfloat16)


def expert_kernel(
    live_ref, outgoing_ref, domains_ref, hidden_ref, expert_in_ref, expert_out_ref,
    mixed_ref,
    inbox, finished, returned, send_sem, recv_sem, back_send, back_recv,
):
    members, capacity, width = outgoing_ref.shape
    hidden_units = expert_out_ref.shape[1]
    rows = hidden_ref.shape[0]
    group = lax.axis_index("seq")
    me = lax.axis_index("emb")

    barrier = pltpu.get_barrier_semaphore()
    for offset in range(1, members):
        pl.semaphore_signal(
            barrier, inc=1, device_id=(group, lax.rem(me + offset, members)), device_id_type=MESH
        )
    pl.semaphore_wait(barrier, members - 1)

    def dispatch(place):
        target = lax.rem(me + ORDER[place], members)
        return pltpu.make_async_remote_copy(
            src_ref=outgoing_ref.at[target],
            dst_ref=inbox.at[place],
            send_sem=send_sem.at[place],
            recv_sem=recv_sem.at[place],
            device_id=(group, target),
            device_id_type=MESH,
        )

    def give_back(place):
        target = lax.rem(me + members - ORDER[place], members)
        return pltpu.make_async_remote_copy(
            src_ref=finished.at[place],
            dst_ref=returned.at[me],
            send_sem=back_send.at[place],
            recv_sem=back_recv.at[place],
            device_id=(group, target),
            device_id_type=MESH,
        )

    remote = [place for place in range(members) if ORDER[place] != 0]
    home = ORDER.index(0)
    for place in remote:
        dispatch(place).start()
    inbox[home] = outgoing_ref[me]

    batch = 4
    tile = 256
    slots = slot_numbers(domains_ref[...], members, capacity)
    same = lax.broadcasted_iota(jnp.int32, (rows, rows), 0) == lax.broadcasted_iota(jnp.int32, (rows, rows), 1)
    slot_column = jnp.sum(jnp.where(same, slots, 0.0), axis=1, keepdims=True).astype(jnp.int32)
    for first in range(0, members, batch):
        places = [place for place in range(first, first + batch) if place != home]
        for place in places:
            dispatch(place).wait_recv()
        taken = inbox[pl.ds(first, batch)].reshape(batch * capacity, width)

        def expert(index, result):
            start = pl.multiple_of(index * tile, tile)
            gate = jnp.dot(taken, expert_in_ref[0, :, pl.ds(start, tile)], preferred_element_type=jnp.float32)
            lift = jnp.dot(
                taken, expert_in_ref[0, :, pl.ds(pl.multiple_of(hidden_units + start, tile), tile)],
                preferred_element_type=jnp.float32,
            )
            activated = (silu(gate) * lift).astype(jnp.bfloat16)
            return result + jnp.dot(
                activated, expert_out_ref[0, pl.ds(start, tile), :], preferred_element_type=jnp.float32
            )

        produced = lax.fori_loop(
            0, hidden_units // tile, expert, jnp.zeros((batch * capacity, width), jnp.float32)
        ).astype(jnp.bfloat16)
        finished[pl.ds(first, batch)] = produced.reshape(batch, capacity, width)
        for place in places:
            give_back(place).start()

    returned[me] = finished[home]
    for place in remote:
        give_back(place).wait_recv()

    number = lax.broadcasted_iota(jnp.int32, (rows, members * capacity), 1)
    chosen = jnp.where(number == slot_column, 1.0, 0.0).astype(jnp.bfloat16)
    expert_rows = jnp.dot(
        chosen, returned[...].reshape(members * capacity, width), preferred_element_type=jnp.float32
    )
    live = lax.broadcasted_iota(jnp.int32, (rows, width), 0) < live_ref[0]
    mixed_ref[...] = jnp.where(live, hidden_ref[...] + expert_rows, 0.0).astype(jnp.bfloat16)
    for place in remote:
        dispatch(place).wait_send()
        give_back(place).wait_send()


def gather_kernel(listed_ref, table_ref, outgoing_ref, place_ref, spread, stage, place_sem):
    load = pltpu.make_async_copy(listed_ref, place_ref, place_sem)
    load.start()
    features, vocabulary = table_ref.shape
    copies = 128 // features
    depth = vocabulary // copies
    members, lines, _ = outgoing_ref.shape

    def arrange(index, carry):
        for step in range(4):
            turn(pl.multiple_of(index * 512 + step * 128, 128))
        return carry

    def turn(start):
        stacked = jnp.concatenate(
            [table_ref[:, pl.ds(pl.multiple_of(k * depth + start, 128), 128)] for k in range(copies)], axis=0
        )
        turned = stacked.astype(jnp.float32).T
        for shift in range(copies):
            moved = turned if shift == 0 else pltpu.roll(turned, shift * features, 1)
            spread[pl.ds(pl.multiple_of(shift * depth + start, 128), 128), :] = moved

    lax.fori_loop(0, depth // 512, arrange, 0)
    load.wait()

    lane = lax.broadcasted_iota(jnp.int32, (1, 128), 1)
    inside = [lane < (k + 1) * features for k in range(copies - 1)]

    def member(target, carry):
        def some(index, carry):
            first = target * (copies * lines) + index * 32
            for line in range(32):
                found = [
                    spread[pl.ds(place_ref[first + k * lines + line], 1), :] for k in range(copies)
                ]
                row = found[-1]
                for k in reversed(range(copies - 1)):
                    row = jnp.where(inside[k], found[k], row)
                stage[pl.ds(index * 32 + line, 1), :] = row
            return carry

        lax.fori_loop(0, lines // 32, some, 0)
        outgoing_ref[target] = stage[...].astype(jnp.bfloat16)
        return carry

    lax.fori_loop(0, members, member, 0)


def exchange_kernel(live_ref, outgoing_ref, gains_ref, embedded_ref, normed_ref, inbox, send_sem, recv_sem):
    members, lines, _ = outgoing_ref.shape
    width = embedded_ref.shape[1]
    features = width // members
    copies = 128 // features
    group = lax.axis_index("seq")
    me = lax.axis_index("emb")

    barrier = pltpu.get_barrier_semaphore()
    for offset in range(1, members):
        pl.semaphore_signal(
            barrier, inc=1, device_id=(group, lax.rem(me + offset, members)), device_id_type=MESH
        )
    pl.semaphore_wait(barrier, members - 1)

    def transfer(place):
        target = lax.rem(me + ORDER[place], members)
        return pltpu.make_async_remote_copy(
            src_ref=outgoing_ref.at[target],
            dst_ref=inbox.at[me],
            send_sem=send_sem.at[place],
            recv_sem=recv_sem.at[place],
            device_id=(group, target),
            device_id_type=MESH,
        )

    remote = [place for place in range(members) if ORDER[place] != 0]
    for place in remote:
        transfer(place).start()
    inbox[me] = outgoing_ref[me]
    for place in remote:
        transfer(place).wait_recv()

    lane = lax.broadcasted_iota(jnp.int32, (lines, 128), 1)
    row = lax.broadcasted_iota(jnp.int32, (lines, 1), 0)
    for part in range(copies):
        blocks = []
        for column in range(width // 128):
            joined = None
            for k in reversed(range(copies)):
                piece = inbox[column * copies + k].astype(jnp.float32)
                shift = (k - part) % copies
                if shift:
                    piece = pltpu.roll(piece, shift * features, 1)
                joined = piece if joined is None else jnp.where(lane < (k + 1) * features, piece, joined)
            blocks.append(joined)
        values = jnp.concatenate(blocks, axis=1)
        span = pl.ds(part * lines, lines)
        embedded_ref[span, :] = values.astype(jnp.bfloat16)
        live = jnp.where(row + part * lines < live_ref[0], 1.0, 0.0)
        normed_ref[span, :] = (rms_norm(values, gains_ref[0:1, :]) * live).astype(jnp.bfloat16)
    for place in remote:
        transfer(place).wait_send()


VMEM = pl.BlockSpec(memory_space=pltpu.VMEM)
SMEM = pl.BlockSpec(memory_space=pltpu.SMEM)


def body(
    item_ids, domains, live_counts, table, norm_gains, proj_in, proj_out, expert_in, expert_out
):
    rows = domains.shape[0]
    width = proj_out.shape[0]
    members = lax.axis_size("emb")
    capacity = 2 * rows // members
    slots = members * capacity

    vocabulary, features = table.shape
    copies = 128 // features
    depth = vocabulary // copies
    lines = rows // copies
    quarter = (jnp.arange(item_ids.shape[0], dtype=jnp.int32) // lines) % copies
    place = ((quarter - item_ids // depth) % copies) * depth + item_ids % depth
    columns = pl.pallas_call(
        gather_kernel,
        out_shape=jax.ShapeDtypeStruct((members, lines, 128), jnp.bfloat16),
        in_specs=[pl.BlockSpec(memory_space=pl.ANY), VMEM],
        out_specs=VMEM,
        scratch_shapes=[
            pltpu.SMEM(item_ids.shape, jnp.int32),
            pltpu.VMEM((copies * depth, 128), jnp.float32),
            pltpu.VMEM((lines, 128), jnp.float32),
            pltpu.SemaphoreType.DMA(()),
        ],
        compiler_params=pltpu.CompilerParams(vmem_limit_bytes=32 << 20),
        name="gather",
    )(place, table.T)
    embedded, normed = pl.pallas_call(
        exchange_kernel,
        out_shape=(jax.ShapeDtypeStruct((rows, width), jnp.bfloat16),) * 2,
        in_specs=[SMEM, VMEM, VMEM],
        out_specs=(VMEM, VMEM),
        scratch_shapes=[
            pltpu.VMEM((members, lines, 128), jnp.bfloat16),
            pltpu.SemaphoreType.DMA((members,)),
            pltpu.SemaphoreType.DMA((members,)),
        ],
        compiler_params=pltpu.CompilerParams(
            collective_id=2, has_side_effects=True, vmem_limit_bytes=12 << 20
        ),
        name="exchange",
    )(live_counts, columns, norm_gains)

    half = rows // 2
    pairs = width // 128
    hidden, outgoing = pl.pallas_call(
        attention_kernel,
        out_shape=(
            jax.ShapeDtypeStruct((rows, width), jnp.float32),
            jax.ShapeDtypeStruct((slots, width), jnp.bfloat16),
        ),
        in_specs=[VMEM] * 6,
        out_specs=(VMEM, VMEM),
        scratch_shapes=[
            pltpu.VMEM((2, SPAN, 2, half, width), jnp.bfloat16),
            pltpu.VMEM((pairs, rows, 128), jnp.bfloat16),
            pltpu.VMEM((rows, width), jnp.float32),
            pltpu.VMEM((pairs, rows, 128), jnp.bfloat16),
            pltpu.VMEM((pairs, rows, 128), jnp.bfloat16),
            pltpu.VMEM((pairs, rows, 128), jnp.float32),
            pltpu.SemaphoreType.DMA((2, SPAN, 2)),
            pltpu.SemaphoreType.DMA((2, SPAN, 2)),
        ],
        compiler_params=pltpu.CompilerParams(
            collective_id=0, has_side_effects=True, vmem_limit_bytes=24 << 20
        ),
        name="attention",
    )(normed, embedded, norm_gains, proj_in, proj_out, domains[None, :])

    return pl.pallas_call(
        expert_kernel,
        out_shape=jax.ShapeDtypeStruct((rows, width), jnp.bfloat16),
        in_specs=[
            SMEM, VMEM, VMEM, VMEM, VMEM, VMEM,
        ],
        out_specs=VMEM,
        scratch_shapes=[
            pltpu.VMEM((members, capacity, width), jnp.bfloat16),
            pltpu.VMEM((members, capacity, width), jnp.bfloat16),
            pltpu.VMEM((members, capacity, width), jnp.bfloat16),
            pltpu.SemaphoreType.DMA((members,)),
            pltpu.SemaphoreType.DMA((members,)),
            pltpu.SemaphoreType.DMA((members,)),
            pltpu.SemaphoreType.DMA((members,)),
        ],
        compiler_params=pltpu.CompilerParams(
            collective_id=1, has_side_effects=True, vmem_limit_bytes=24 << 20
        ),
        name="experts",
    )(
        live_counts, outgoing.reshape(members, capacity, width), domains[None, :], hidden,
        expert_in, expert_out,
    )


def solution(mesh):
    in_specs = (
        P("seq"),
        P(("seq", "emb")),
        P(("seq", "emb")),
        P(None, "emb"),
        P(),
        P(),
        P(),
        P("emb", None, None),
        P("emb", None, None),
    )
    out_specs = P(("seq", "emb"), None)
    return jax.shard_map(body, mesh=mesh, in_specs=in_specs, out_specs=out_specs, check_vma=False)
```

```python
import math

import jax
import jax.numpy as jnp
from jax import lax
from jax.experimental import pallas as pl
from jax.experimental.pallas import tpu as pltpu
from jax.sharding import PartitionSpec as P

HEADS = 8
HEAD_DIM = 64
SPAN = 4
MESH = pl.DeviceIdType.MESH

norm_eps = 1e-06

ORDER = (4, 12, 3, 13, 5, 11, 2, 14, 6, 10, 1, 15, 7, 9, 8, 0)


def rms_norm(values, gain):
    return values * lax.rsqrt(jnp.mean(values * values, axis=-1, keepdims=True) + norm_eps) * gain


def silu(values):
    return values * (0.5 * jnp.tanh(0.5 * values) + 0.5)


def slot_numbers(domains, members, capacity):
    rows = domains.shape[1]
    onehot = jnp.where(lax.broadcasted_iota(jnp.int32, (members, rows), 0) == domains, 1.0, 0.0)
    before = jnp.where(
        lax.broadcasted_iota(jnp.int32, (rows, rows), 0) < lax.broadcasted_iota(jnp.int32, (rows, rows), 1),
        1.0, 0.0,
    )
    ranks = jnp.dot(
        onehot.astype(jnp.bfloat16), before.astype(jnp.bfloat16), preferred_element_type=jnp.float32
    )
    rank = jnp.sum(ranks * onehot, axis=0, keepdims=True)
    return domains.astype(jnp.float32) * capacity + rank


def attention_kernel(
    normed_ref, embedded_ref, gains_ref, proj_in_ref, proj_out_ref, domains_ref,
    hidden_ref, outgoing_ref,
    halo, queries, gating, keys, values, total, send_sem, recv_sem,
):
    rows, width = normed_ref.shape
    half = rows // 2
    pairs = width // 128
    groups, members = lax.axis_size("seq"), lax.axis_size("emb")
    count = groups * members
    me = lax.axis_index("seq") * members + lax.axis_index("emb")
    right = lax.rem(me + 1, count)
    left = lax.rem(me + count - 1, count)
    targets = [
        (lax.div(right, members), lax.rem(right, members)),
        (lax.div(left, members), lax.rem(left, members)),
    ]

    barrier = pltpu.get_barrier_semaphore()
    for target in targets:
        pl.semaphore_signal(barrier, inc=1, device_id=target, device_id_type=MESH)
    pl.semaphore_wait(barrier, 2)

    def transfer(way, distance, part, source):
        slot = (way, distance, part)
        return pltpu.make_async_remote_copy(
            src_ref=source,
            dst_ref=halo.at[slot],
            send_sem=send_sem.at[slot],
            recv_sem=recv_sem.at[slot],
            device_id=targets[way],
            device_id_type=MESH,
        )

    for part in range(2):
        for way in range(2):
            transfer(way, 0, part, normed_ref.at[pl.ds(part * half, half)]).start()

    normed = normed_ref[...]
    for pair in range(pairs):
        columns = pl.ds(pair * 128, 128)
        gate = jnp.dot(normed, proj_in_ref[:, columns], preferred_element_type=jnp.float32)
        gating[:, columns] = silu(gate)
        query = jnp.dot(
            normed, proj_in_ref[:, pl.ds(width + pair * 128, 128)], preferred_element_type=jnp.float32
        ).astype(jnp.bfloat16)
        queries[pair] = query * jnp.bfloat16(0.5 / math.sqrt(HEAD_DIM))
        total[pair] = jnp.zeros((rows, 128), jnp.float32)

    slot_row = slot_numbers(domains_ref[...], members, outgoing_ref.shape[0] // members).astype(jnp.int32)
    low_lanes = lax.broadcasted_iota(jnp.int32, (half, 128), 1) < HEAD_DIM

    def attend(block, tiles):
        def project(group, carry):
            for base, held in ((2 * width, keys), (3 * width, values)):
                columns = pl.ds(pl.multiple_of(base + group * 256, 256), 256)
                found = jnp.dot(block, proj_in_ref[:, columns], preferred_element_type=jnp.float32)
                for side in range(2):
                    pair = 2 * group + side
                    mine = found[:, side * 128 : (side + 1) * 128]
                    held[pair, pl.ds(0, half), :] = jnp.where(low_lanes, mine, 0.0).astype(jnp.bfloat16)
                    held[pair, pl.ds(half, half), :] = jnp.where(low_lanes, 0.0, mine).astype(jnp.bfloat16)
            return carry

        lax.fori_loop(0, pairs // 2, project, 0)

        def weigh(pair, carry):
            for tile, band in tiles:
                span = pl.ds(tile * half, half)
                scores = lax.dot_general(
                    queries[pair, span, :], keys[pair], (((1,), (1,)), ((), ())),
                    preferred_element_type=jnp.float32,
                )
                weights = scores * jnp.tanh(scores) + scores
                if band is not None:
                    row = lax.broadcasted_iota(jnp.int32, scores.shape, 0)
                    column = lax.broadcasted_iota(jnp.int32, scores.shape, 1) & (half - 1)
                    weights = jnp.where(column >= row if band == 0 else column <= row, weights, 0.0)
                total[pair, span, :] += jnp.dot(
                    weights.astype(jnp.bfloat16), values[pair], preferred_element_type=jnp.float32
                )
            return carry

        lax.fori_loop(0, pairs, weigh, 0)

    everything = ((0, None), (1, None))

    def own(part, carry):
        attend(normed_ref[pl.ds(pl.multiple_of(part * half, half), half), :], everything)
        return carry

    lax.fori_loop(0, 2, own, 0)

    def in_range(way, distance):
        return me - distance > 0 if way == 0 else me + distance < count - 1

    def step(index, carry):
        distance, part = lax.div(index, 2), lax.rem(index, 2)
        for way in range(2):
            arrived = halo.at[way, distance, part]
            transfer(way, distance, part, arrived).wait_recv()
            transfer(way, distance + 1, part, arrived).start()

        def one(way, carry):
            inside = jnp.where(way == 0, me - distance > 0, me + distance < count - 1)

            @pl.when(inside)
            def _():
                attend(halo[way, distance, part], everything)

            return carry

        lax.fori_loop(0, 2, one, 0)
        return carry

    lax.fori_loop(0, 2 * (SPAN - 1), step, 0)

    last = SPAN - 1
    edge_tiles = (
        (((0, 0),), ((0, 1), (1, None))),
        (((0, None), (1, 0)), ((1, 1),)),
    )
    for part in range(2):
        for way in range(2):
            transfer(way, last, part, halo.at[way, last, part]).wait_recv()

            @pl.when(in_range(way, last))
            def _():
                attend(halo[way, last, part], edge_tiles[part][way])

    def settle(index, carry):
        distance, part = lax.div(index, 2), lax.rem(index, 2)
        for way in range(2):
            transfer(way, distance, part, halo.at[way, distance, part]).wait_send()
        return carry

    lax.fori_loop(0, 2 * SPAN, settle, 0)

    attended = jnp.concatenate([total[pair] for pair in range(pairs)], axis=1)
    gated = (rms_norm(attended, gains_ref[1:2, :]) * gating[...]).astype(jnp.bfloat16)
    hidden = embedded_ref[...].astype(jnp.float32) + jnp.dot(
        gated, proj_out_ref[...], preferred_element_type=jnp.float32
    )
    hidden_ref[...] = hidden
    routed = rms_norm(hidden, gains_ref[2:3, :]).astype(jnp.bfloat16)
    slots = outgoing_ref.shape[0]
    chunk = 256
    for first in range(0, slots, chunk):
        number = lax.broadcasted_iota(jnp.int32, (chunk, rows), 0) + first
        chosen = jnp.where(number == slot_row, 1.0, 0.0).astype(jnp.bfloat16)
        outgoing_ref[pl.ds(first, chunk), :] = jnp.dot(
            chosen, routed, preferred_element_type=jnp.float32
        ).astype(jnp.bfloat16)


def expert_kernel(
    live_ref, outgoing_ref, domains_ref, hidden_ref, expert_in_ref, expert_out_ref,
    mixed_ref,
    inbox, finished, returned, send_sem, recv_sem, back_send, back_recv,
):
    members, capacity, width = outgoing_ref.shape
    hidden_units = expert_out_ref.shape[1]
    rows = hidden_ref.shape[0]
    group = lax.axis_index("seq")
    me = lax.axis_index("emb")

    barrier = pltpu.get_barrier_semaphore()
    for offset in range(1, members):
        pl.semaphore_signal(
            barrier, inc=1, device_id=(group, lax.rem(me + offset, members)), device_id_type=MESH
        )
    pl.semaphore_wait(barrier, members - 1)

    def dispatch(place):
        target = lax.rem(me + ORDER[place], members)
        return pltpu.make_async_remote_copy(
            src_ref=outgoing_ref.at[target],
            dst_ref=inbox.at[place],
            send_sem=send_sem.at[place],
            recv_sem=recv_sem.at[place],
            device_id=(group, target),
            device_id_type=MESH,
        )

    def give_back(place):
        target = lax.rem(me + members - ORDER[place], members)
        return pltpu.make_async_remote_copy(
            src_ref=finished.at[place],
            dst_ref=returned.at[me],
            send_sem=back_send.at[place],
            recv_sem=back_recv.at[place],
            device_id=(group, target),
            device_id_type=MESH,
        )

    remote = [place for place in range(members) if ORDER[place] != 0]
    home = ORDER.index(0)
    for place in remote:
        dispatch(place).start()
    inbox[home] = outgoing_ref[me]

    batch = 4
    tile = 256
    slots = slot_numbers(domains_ref[...], members, capacity)
    same = lax.broadcasted_iota(jnp.int32, (rows, rows), 0) == lax.broadcasted_iota(jnp.int32, (rows, rows), 1)
    slot_column = jnp.sum(jnp.where(same, slots, 0.0), axis=1, keepdims=True).astype(jnp.int32)
    for first in range(0, members, batch):
        places = [place for place in range(first, first + batch) if place != home]
        for place in places:
            dispatch(place).wait_recv()
        taken = inbox[pl.ds(first, batch)].reshape(batch * capacity, width)

        def expert(index, result):
            start = pl.multiple_of(index * tile, tile)
            gate = jnp.dot(taken, expert_in_ref[0, :, pl.ds(start, tile)], preferred_element_type=jnp.float32)
            lift = jnp.dot(
                taken, expert_in_ref[0, :, pl.ds(pl.multiple_of(hidden_units + start, tile), tile)],
                preferred_element_type=jnp.float32,
            )
            activated = (silu(gate) * lift).astype(jnp.bfloat16)
            return result + jnp.dot(
                activated, expert_out_ref[0, pl.ds(start, tile), :], preferred_element_type=jnp.float32
            )

        produced = lax.fori_loop(
            0, hidden_units // tile, expert, jnp.zeros((batch * capacity, width), jnp.float32)
        ).astype(jnp.bfloat16)
        finished[pl.ds(first, batch)] = produced.reshape(batch, capacity, width)
        for place in places:
            give_back(place).start()

    returned[me] = finished[home]
    for place in remote:
        give_back(place).wait_recv()

    number = lax.broadcasted_iota(jnp.int32, (rows, members * capacity), 1)
    chosen = jnp.where(number == slot_column, 1.0, 0.0).astype(jnp.bfloat16)
    expert_rows = jnp.dot(
        chosen, returned[...].reshape(members * capacity, width), preferred_element_type=jnp.float32
    )
    live = lax.broadcasted_iota(jnp.int32, (rows, width), 0) < live_ref[0]
    mixed_ref[...] = jnp.where(live, hidden_ref[...] + expert_rows, 0.0).astype(jnp.bfloat16)
    for place in remote:
        dispatch(place).wait_send()
        give_back(place).wait_send()


def gather_kernel(listed_ref, table_ref, outgoing_ref, place_ref, spread, stage, place_sem):
    load = pltpu.make_async_copy(listed_ref, place_ref, place_sem)
    load.start()
    features, vocabulary = table_ref.shape
    copies = 128 // features
    depth = vocabulary // copies
    members, lines, _ = outgoing_ref.shape

    def arrange(index, carry):
        for step in range(4):
            turn(pl.multiple_of(index * 512 + step * 128, 128))
        return carry

    def turn(start):
        stacked = jnp.concatenate(
            [table_ref[:, pl.ds(pl.multiple_of(k * depth + start, 128), 128)] for k in range(copies)], axis=0
        )
        turned = stacked.astype(jnp.float32).T
        for shift in range(copies):
            moved = turned if shift == 0 else pltpu.roll(turned, shift * features, 1)
            spread[pl.ds(pl.multiple_of(shift * depth + start, 128), 128), :] = moved

    lax.fori_loop(0, depth // 512, arrange, 0)
    load.wait()

    lane = lax.broadcasted_iota(jnp.int32, (1, 128), 1)
    inside = [lane < (k + 1) * features for k in range(copies - 1)]

    def member(target, carry):
        def some(index, carry):
            first = target * (copies * lines) + index * 32
            for line in range(32):
                found = [
                    spread[pl.ds(place_ref[first + k * lines + line], 1), :] for k in range(copies)
                ]
                row = found[-1]
                for k in reversed(range(copies - 1)):
                    row = jnp.where(inside[k], found[k], row)
                stage[pl.ds(index * 32 + line, 1), :] = row
            return carry

        lax.fori_loop(0, lines // 32, some, 0)
        outgoing_ref[target] = stage[...].astype(jnp.bfloat16)
        return carry

    lax.fori_loop(0, members, member, 0)


def exchange_kernel(live_ref, outgoing_ref, gains_ref, embedded_ref, normed_ref, inbox, send_sem, recv_sem):
    members, lines, _ = outgoing_ref.shape
    width = embedded_ref.shape[1]
    features = width // members
    copies = 128 // features
    group = lax.axis_index("seq")
    me = lax.axis_index("emb")

    barrier = pltpu.get_barrier_semaphore()
    for offset in range(1, members):
        pl.semaphore_signal(
            barrier, inc=1, device_id=(group, lax.rem(me + offset, members)), device_id_type=MESH
        )
    pl.semaphore_wait(barrier, members - 1)

    def transfer(place):
        target = lax.rem(me + ORDER[place], members)
        return pltpu.make_async_remote_copy(
            src_ref=outgoing_ref.at[target],
            dst_ref=inbox.at[me],
            send_sem=send_sem.at[place],
            recv_sem=recv_sem.at[place],
            device_id=(group, target),
            device_id_type=MESH,
        )

    remote = [place for place in range(members) if ORDER[place] != 0]
    for place in remote:
        transfer(place).start()
    inbox[me] = outgoing_ref[me]
    for place in remote:
        transfer(place).wait_recv()

    lane = lax.broadcasted_iota(jnp.int32, (lines, 128), 1)
    row = lax.broadcasted_iota(jnp.int32, (lines, 1), 0)
    for part in range(copies):
        blocks = []
        for column in range(width // 128):
            joined = None
            for k in reversed(range(copies)):
                piece = inbox[column * copies + k].astype(jnp.float32)
                shift = (k - part) % copies
                if shift:
                    piece = pltpu.roll(piece, shift * features, 1)
                joined = piece if joined is None else jnp.where(lane < (k + 1) * features, piece, joined)
            blocks.append(joined)
        values = jnp.concatenate(blocks, axis=1)
        span = pl.ds(part * lines, lines)
        embedded_ref[span, :] = values.astype(jnp.bfloat16)
        live = jnp.where(row + part * lines < live_ref[0], 1.0, 0.0)
        normed_ref[span, :] = (rms_norm(values, gains_ref[0:1, :]) * live).astype(jnp.bfloat16)
    for place in remote:
        transfer(place).wait_send()


VMEM = pl.BlockSpec(memory_space=pltpu.VMEM)
SMEM = pl.BlockSpec(memory_space=pltpu.SMEM)


def body(
    item_ids, domains, live_counts, table, norm_gains, proj_in, proj_out, expert_in, expert_out
):
    rows = domains.shape[0]
    width = proj_out.shape[0]
    members = lax.axis_size("emb")
    capacity = 2 * rows // members
    slots = members * capacity

    vocabulary, features = table.shape
    copies = 128 // features
    depth = vocabulary // copies
    lines = rows // copies
    quarter = (jnp.arange(item_ids.shape[0], dtype=jnp.int32) // lines) % copies
    place = ((quarter - item_ids // depth) % copies) * depth + item_ids % depth
    columns = pl.pallas_call(
        gather_kernel,
        out_shape=jax.ShapeDtypeStruct((members, lines, 128), jnp.bfloat16),
        in_specs=[pl.BlockSpec(memory_space=pl.ANY), VMEM],
        out_specs=VMEM,
        scratch_shapes=[
            pltpu.SMEM(item_ids.shape, jnp.int32),
            pltpu.VMEM((copies * depth, 128), jnp.float32),
            pltpu.VMEM((lines, 128), jnp.float32),
            pltpu.SemaphoreType.DMA(()),
        ],
        compiler_params=pltpu.CompilerParams(vmem_limit_bytes=32 << 20),
        name="gather",
    )(place, table.T)
    embedded, normed = pl.pallas_call(
        exchange_kernel,
        out_shape=(jax.ShapeDtypeStruct((rows, width), jnp.bfloat16),) * 2,
        in_specs=[SMEM, VMEM, VMEM],
        out_specs=(VMEM, VMEM),
        scratch_shapes=[
            pltpu.VMEM((members, lines, 128), jnp.bfloat16),
            pltpu.SemaphoreType.DMA((members,)),
            pltpu.SemaphoreType.DMA((members,)),
        ],
        compiler_params=pltpu.CompilerParams(
            collective_id=2, has_side_effects=True, vmem_limit_bytes=12 << 20
        ),
        name="exchange",
    )(live_counts, columns, norm_gains)

    half = rows // 2
    pairs = width // 128
    hidden, outgoing = pl.pallas_call(
        attention_kernel,
        out_shape=(
            jax.ShapeDtypeStruct((rows, width), jnp.float32),
            jax.ShapeDtypeStruct((slots, width), jnp.bfloat16),
        ),
        in_specs=[VMEM] * 6,
        out_specs=(VMEM, VMEM),
        scratch_shapes=[
            pltpu.VMEM((2, SPAN, 2, half, width), jnp.bfloat16),
            pltpu.VMEM((pairs, rows, 128), jnp.bfloat16),
            pltpu.VMEM((rows, width), jnp.float32),
            pltpu.VMEM((pairs, rows, 128), jnp.bfloat16),
            pltpu.VMEM((pairs, rows, 128), jnp.bfloat16),
            pltpu.VMEM((pairs, rows, 128), jnp.float32),
            pltpu.SemaphoreType.DMA((2, SPAN, 2)),
            pltpu.SemaphoreType.DMA((2, SPAN, 2)),
        ],
        compiler_params=pltpu.CompilerParams(
            collective_id=0, has_side_effects=True, vmem_limit_bytes=24 << 20
        ),
        name="attention",
    )(normed, embedded, norm_gains, proj_in, proj_out, domains[None, :])

    return pl.pallas_call(
        expert_kernel,
        out_shape=jax.ShapeDtypeStruct((rows, width), jnp.bfloat16),
        in_specs=[
            SMEM, VMEM, VMEM, VMEM, VMEM, VMEM,
        ],
        out_specs=VMEM,
        scratch_shapes=[
            pltpu.VMEM((members, capacity, width), jnp.bfloat16),
            pltpu.VMEM((members, capacity, width), jnp.bfloat16),
            pltpu.VMEM((members, capacity, width), jnp.bfloat16),
            pltpu.SemaphoreType.DMA((members,)),
            pltpu.SemaphoreType.DMA((members,)),
            pltpu.SemaphoreType.DMA((members,)),
            pltpu.SemaphoreType.DMA((members,)),
        ],
        compiler_params=pltpu.CompilerParams(
            collective_id=1, has_side_effects=True, vmem_limit_bytes=24 << 20
        ),
        name="experts",
    )(
        live_counts, outgoing.reshape(members, capacity, width), domains[None, :], hidden,
        expert_in, expert_out,
    )


def solution(mesh):
    in_specs = (
        P("seq"),
        P(("seq", "emb")),
        P(("seq", "emb")),
        P(None, "emb"),
        P(),
        P(),
        P(),
        P("emb", None, None),
        P("emb", None, None),
    )
    out_specs = P(("seq", "emb"), None)
    return jax.shard_map(body, mesh=mesh, in_specs=in_specs, out_specs=out_specs, check_vma=False)
```
